32 devices in a mesh: sec: 8 (over y, x, core), pan: 4 (over z).
Axes of the slice: x: 2, y: 2, z: 4, core: 2. Of those that a mesh axis runs over, the one named last changes fastest.
Arguments:
- wave_state: bfloat16 [8, 512, 512], P('sec', 'pan'), may hold values from -6 to 6
- right_blocks: bfloat16 [8, 16, 512, 512], P('sec', None, None, 'pan'), may hold values from -0.25 to 0.25
- left_blocks: bfloat16 [576, 512, 512], P('sec', 'pan'), may hold values from -0.125 to 0.125
- coupling: bfloat16 [576], P('sec'), may hold values from -1 to 1
- channel_term: int32 [576], P('sec'), may hold values from 0 to 15
- channel_out: int32 [576], P('sec'), may hold values from 0 to 7, as said below
- sector_dims: int32 [8], P('sec'), may hold values from 128 to 512
Outputs:
- applied: float32 [8, 512, 512], P('sec', 'pan')
The draws below stay inside these ranges and needn't reach their ends.
Inputs may be any that keep to these rules, and one draw needn't show every extreme that they name: `channel_out`: channel c ends in a sector at most two away from the sector c // 72 that it starts from.
All inputs are finite; a program needn't handle non-finite values.
Results may differ from the reference program's by a relative error of at most 0.0041.
Values may be sent and summed in bfloat16 or wider, within the bound.
A program may use at most 128 MiB of HBM per device.

```python
import jax
import jax.numpy as jnp
from jax import lax

DB = 512
NW = 16
CH_DEV = 72
SECTORS = 8
CHANNELS = 576


def draw_channel_out(key, part):
    chan_total = CH_DEV * SECTORS
    source = jnp.arange(chan_total, dtype=jnp.int32) // CH_DEV
    offset = jax.random.randint(key, (chan_total,), -2, 3, dtype=jnp.int32)
    return jnp.clip(source + offset, 0, SECTORS - 1).astype(jnp.int32)


def place_ends(drawn, stream_key, low, largest):
    longest = drawn.shape.index(max(drawn.shape))
    spots = []
    for shift in (0, 1):
        where = [jax.random.randint(jax.random.fold_in(stream_key, axis), (), 0, length) for axis, length in enumerate(drawn.shape)]
        where[longest] = (where[longest] + shift) % drawn.shape[longest]
        spots.append(tuple(where))
    return drawn.at[spots[0]].set(low).at[spots[1]].set(largest)


def block_scale(own_key, shape, pieces, smallest, largest):
    factor_of = 1.0
    for position, shards_of in pieces:
        draws = jax.random.uniform(jax.random.fold_in(jax.random.fold_in(own_key, 6), position), (shards_of,), jnp.float32, smallest / len(pieces), largest / len(pieces))
        factor_of = factor_of * jnp.repeat(jnp.exp(draws), shape[position] // shards_of).reshape((-1,) + (1,) * (len(shape) - 1 - position))
    return factor_of


def bell_draw(rng, extent, spread, reach, shards=(), kind=jnp.bfloat16):
    gain = block_scale(rng, extent, shards, -0.22, 0.18) if shards else 1.0
    drawn = jax.random.normal(rng, extent, jnp.float32) * spread * gain
    return jnp.minimum(jnp.maximum(drawn, -reach), reach).astype(kind)


def setup_inputs(seed: int = 0) -> dict:
    streams_of = jax.random.split(jax.random.key(seed), 8)
    return {
        "wave_state": bell_draw(streams_of[0], (SECTORS, DB, DB), 1.0, 6.0, ((0, 8), (1, 4))),
        "right_blocks": bell_draw(streams_of[1], (SECTORS, NW, DB, DB), DB ** -0.5, 0.25, ((0, 8), (3, 4))),
        "left_blocks": bell_draw(streams_of[2], (CHANNELS, DB, DB), (4 * DB) ** -0.5, 0.125, ((0, 8), (1, 4))),
        "coupling": jnp.clip(jax.random.uniform(streams_of[3], (CHANNELS,), jnp.float32, -1.0, 1.0) * block_scale(streams_of[3], (CHANNELS,), ((0, 8),), -0.4, 0.0), -1.0, 1.0).astype(jnp.bfloat16),
        "channel_term": place_ends(jax.random.randint(streams_of[4], (CHANNELS,), 0, NW), jax.random.fold_in(streams_of[4], 1), 0, NW - 1).astype(jnp.int32),
        "channel_out": draw_channel_out(jax.random.fold_in(streams_of[7], 71), 0),
        "sector_dims": place_ends(jax.random.randint(streams_of[6], (SECTORS,), DB // 4, DB + 1), jax.random.fold_in(streams_of[6], 1), DB // 4, DB).astype(jnp.int32),
    }


def reference(wave_state, right_blocks, left_blocks, coupling, channel_term, channel_out, sector_dims):
    indices = jnp.arange(DB, dtype=jnp.int32)
    slot_ids = jnp.arange(5, dtype=jnp.int32)
    term_ids = jnp.arange(NW, dtype=jnp.int32)

    def visit_sector(totals, sector):
        live_dim = sector_dims[sector]
        inside = (indices[:, None] < live_dim) & (indices[None, :] < live_dim)
        masked = jnp.where(inside, wave_state[sector], jnp.zeros((), jnp.bfloat16))
        terms_here = jnp.einsum("ik,wkq->wiq", masked.astype(jnp.float32), right_blocks[sector].astype(jnp.float32)).astype(jnp.bfloat16)
        first_chan = (sector * CH_DEV).astype(jnp.int32)
        left_part = lax.dynamic_slice_in_dim(left_blocks, first_chan, CH_DEV, 0)
        coef_part = lax.dynamic_slice_in_dim(coupling, first_chan, CH_DEV, 0)
        kind_part = lax.dynamic_slice_in_dim(channel_term, first_chan, CH_DEV, 0)
        targets = lax.dynamic_slice_in_dim(channel_out, first_chan, CH_DEV, 0)
        slot_index = targets - sector + 2
        chosen = (slot_index[None, None, :] == slot_ids[:, None, None]) & (kind_part[None, None, :] == term_ids[None, :, None])
        weights = jnp.where(chosen, coef_part[None, None, :], jnp.zeros((), jnp.bfloat16)).reshape(5 * NW, CH_DEV)
        combined = jnp.dot(weights, left_part.reshape(CH_DEV, DB * DB), preferred_element_type=jnp.float32)
        combined = combined.astype(jnp.bfloat16).reshape(5, NW, DB, DB)
        partial_value = jnp.einsum("jwri,wiq->jrq", combined.astype(jnp.float32), terms_here.astype(jnp.float32))
        window = lax.dynamic_slice_in_dim(totals, sector, 5, 0)
        totals = lax.dynamic_update_slice_in_dim(totals, window + partial_value, sector, 0)
        return totals, None

    start_totals = jnp.zeros((SECTORS + 4, DB, DB), jnp.float32)
    totals, _ = lax.scan(visit_sector, start_totals, jnp.arange(SECTORS, dtype=jnp.int32))
    summed = totals[2:SECTORS + 2]
    limits = sector_dims[:, None, None]
    kept_mask = (indices[None, :, None] < limits) & (indices[None, None, :] < limits)
    return jnp.where(kept_mask, summed, jnp.zeros((), jnp.float32))
```

```python
import functools

import jax
import jax.numpy as jnp
from jax import lax
from jax.experimental import pallas as pl
from jax.experimental.pallas import tpu as pltpu
from jax.sharding import PartitionSpec as P

OFFSETS = (-2, -1, 1, 2)
F32 = jnp.float32
BF16 = jnp.bfloat16


def combine_kernel(cell_ref, coef_ref, left_ref, out_ref, acc_ref):
    acc_ref[...] = jnp.zeros_like(acc_ref)

    @pl.loop(0, left_ref.shape[0])
    def _(channel):
        cell = cell_ref[channel]
        acc_ref[cell] += left_ref[channel].astype(F32) * coef_ref[channel]

    @pl.loop(0, out_ref.shape[0])
    def _(cell):
        out_ref[cell] = acc_ref[cell].astype(BF16)


def combine(cells, coefs, left_blocks, cell_count):
    channels, rows, width = left_blocks.shape
    step = min(rows, 32)
    return pl.pallas_call(
        combine_kernel,
        grid=(rows // step,),
        in_specs=[
            pl.BlockSpec(memory_space=pltpu.SMEM),
            pl.BlockSpec(memory_space=pltpu.SMEM),
            pl.BlockSpec((channels, step, width), lambda i: (0, i, 0)),
        ],
        out_specs=pl.BlockSpec((cell_count, step, width), lambda i: (0, i, 0)),
        out_shape=jax.ShapeDtypeStruct((cell_count, rows, width), BF16),
        scratch_shapes=[pltpu.VMEM((cell_count, step, width), F32)],
        compiler_params=pltpu.CompilerParams(vmem_limit_bytes=48 * 2**20),
    )(cells, coefs, left_blocks)


def line_kernel(
    sectors, moved, dims_ref, state_ref, right_ref, comb_ref, out_ref,
    state_all, masked, gathered, comb, comb_end, acc, acc_end,
    stage, landed, stage_end, landed_end, back, back_landed,
    local_sems, state_send, state_recv, own_send, relay_send, right_recv,
    end_send, end_recv, part_send, part_recv, part_end_send, part_end_recv, back_sems,
):
    terms, width, cols = right_ref.shape
    rows = state_ref.shape[0]
    me = lax.axis_index("pan")
    sector = lax.axis_index("sec")
    is_mid = (me == 1) | (me == 2)
    is_end = jnp.logical_not(is_mid)
    near_end = jnp.where(me <= 1, 0, 3)
    other_mid = jnp.where(me <= 1, 2, 1)
    far_end = 3 - near_end
    near_mid = jnp.where(me <= 1, 1, 2)

    def remote(src, dst, send, recv, where, axis="pan"):
        return pltpu.make_async_remote_copy(
            src_ref=src, dst_ref=dst, send_sem=send, recv_sem=recv,
            device_id={axis: where}, device_id_type=pl.DeviceIdType.MESH,
        )

    def state_copy(shift):
        where = lax.rem(me + shift, 4)
        spot = state_all.at[me]
        return remote(state_ref, spot, state_send.at[shift], state_recv.at[me], where)

    def state_wait(owner):
        remote(state_ref, state_all.at[owner], state_send.at[0], state_recv.at[owner], me).wait_recv()

    def own_copy(way, term, where):
        return remote(
            right_ref.at[term], gathered.at[me, term],
            own_send.at[way, term], right_recv.at[me, term], where,
        )

    def relay_copy(way, owner, term, where):
        block = gathered.at[owner, term]
        return remote(block, block, relay_send.at[way, term], right_recv.at[owner, term], where)

    def end_copy(term):
        return remote(comb_ref.at[term], comb_end.at[term], end_send.at[term], end_recv.at[term], near_mid)

    def arrived(owner, term):
        block = gathered.at[owner, term]
        remote(block, block, relay_send.at[0, term], right_recv.at[owner, term], me).wait_recv()

    def part_copy(index, owner):
        return remote(
            stage.at[index, owner], landed.at[index, owner],
            part_send.at[index, owner], part_recv.at[index, owner], sector + OFFSETS[index], "sec",
        )

    def part_end_copy(index):
        return remote(
            stage_end.at[index], landed_end.at[index],
            part_end_send.at[index], part_end_recv.at[index], sector + OFFSETS[index], "sec",
        )

    def goes(index):
        target = sector + OFFSETS[index]
        return (target >= 0) & (target < sectors)

    def comes(index):
        source = sector - OFFSETS[index]
        return (source >= 0) & (source < sectors)

    for shift in (1, 2, 3):
        state_copy(shift).start()

    @pl.when(is_mid)
    def _():
        @pl.loop(0, terms)
        def _(term):
            own_copy(0, term, other_mid).start()

            @pl.when(term >= moved)
            def _():
                own_copy(1, term, near_end).start()

    @pl.when(is_end)
    def _():
        @pl.loop(0, terms)
        def _(term):
            own_copy(0, term, near_mid).start()

        @pl.loop(0, moved)
        def _(term):
            end_copy(term).start()

    copies = [
        pltpu.make_async_copy(state_ref, state_all.at[me], local_sems.at[0]),
        pltpu.make_async_copy(right_ref, gathered.at[me], local_sems.at[1]),
        pltpu.make_async_copy(comb_ref, comb, local_sems.at[2]),
    ]
    for copy in copies:
        copy.start()
    acc[...] = jnp.zeros_like(acc)
    acc_end[...] = jnp.zeros_like(acc_end)
    for copy in copies:
        copy.wait()
    for shift in (1, 2, 3):
        state_wait(lax.rem(me + shift, 4))
    live = dims_ref[0]
    inside_col = lax.broadcasted_iota(jnp.int32, (rows, width), 1) < live
    for owner in range(4):
        row = lax.broadcasted_iota(jnp.int32, (rows, width), 0) + owner * rows
        masked[owner * rows:(owner + 1) * rows, :] = jnp.where(
            inside_col & (row < live), state_all[owner].astype(F32), 0.0
        ).astype(BF16)

    def multiply(owner, term, left, total):
        block = jnp.dot(masked[...], gathered[owner, term], preferred_element_type=F32).astype(BF16)
        total[owner] += jnp.dot(left[term], block, preferred_element_type=F32)

    def send_parts(owner):
        for index in range(4):
            slot = OFFSETS[index] + 2

            @pl.when(goes(index))
            def _():
                stage[index, owner] = acc[owner, slot * rows:(slot + 1) * rows, :].astype(BF16)
                part_copy(index, owner).start()

    @pl.when(is_mid)
    def _():
        @pl.loop(0, terms)
        def _(term):
            arrived(other_mid, term)

            @pl.when(term >= moved)
            def _():
                relay_copy(0, other_mid, term, near_end).start()

            arrived(near_end, term)
            relay_copy(1, near_end, term, other_mid).start()

            @pl.loop(0, 3)
            def _(which):
                owner = jnp.where(which == 0, me, jnp.where(which == 1, other_mid, near_end))
                multiply(owner, term, comb, acc)

        @pl.loop(0, 3)
        def _(which):
            send_parts(jnp.where(which == 0, me, jnp.where(which == 1, other_mid, near_end)))

        @pl.loop(0, terms)
        def _(term):
            arrived(far_end, term)

            @pl.when(term >= moved)
            def _():
                relay_copy(2, far_end, term, near_end).start()

            multiply(far_end, term, comb, acc)

        send_parts(far_end)

        @pl.loop(0, moved)
        def _(term):
            remote(comb_ref.at[term], comb_end.at[term], end_send.at[term], end_recv.at[term], me).wait_recv()

            @pl.loop(0, 4)
            def _(owner):
                multiply(owner, term, comb_end, acc_end)

        for index in range(4):
            slot = OFFSETS[index] + 2

            @pl.when(goes(index))
            def _():
                stage_end[index] = acc_end[:, slot * rows:(slot + 1) * rows, :].astype(BF16)
                part_end_copy(index).start()

        for index in range(4):
            @pl.when(comes(index))
            def _():
                part_end_copy(index).wait_recv()
                acc_end[:, 2 * rows:3 * rows, :] += landed_end[index].astype(F32)

        back[...] = acc_end[:, 2 * rows:3 * rows, :].astype(BF16)
        remote(back, back_landed, back_sems.at[0], back_sems.at[1], near_end).start()

    @pl.when(is_end)
    def _():
        turn = jnp.where(me == 0, 1, -1)

        @pl.loop(0, 4)
        def _(rank):
            owner = me + turn * rank

            @pl.loop(moved, terms)
            def _(term):
                @pl.when(rank > 0)
                def _():
                    arrived(owner, term)

                multiply(owner, term, comb, acc)

            send_parts(owner)

    for index in range(4):
        @pl.when(comes(index))
        def _():
            @pl.loop(0, 4)
            def _(owner):
                part_copy(index, owner).wait_recv()
                acc[owner, 2 * rows:3 * rows, :] += landed[index, owner].astype(F32)

    @pl.when(is_end)
    def _():
        remote(back, back_landed, back_sems.at[0], back_sems.at[1], me).wait_recv()
        acc[:, 2 * rows:3 * rows, :] += back_landed[...].astype(F32)

    for owner in range(4):
        out_ref[:, owner * cols:(owner + 1) * cols] = acc[owner, 2 * rows:3 * rows, :]

    for shift in (1, 2, 3):
        state_copy(shift).wait_send()
    for index in range(4):
        @pl.when(goes(index))
        def _():
            @pl.loop(0, 4)
            def _(owner):
                part_copy(index, owner).wait_send()

            @pl.when(is_mid)
            def _():
                part_end_copy(index).wait_send()

    @pl.when(is_mid)
    def _():
        @pl.loop(0, terms)
        def _(term):
            own_copy(0, term, other_mid).wait_send()
            relay_copy(1, near_end, term, other_mid).wait_send()

            @pl.when(term >= moved)
            def _():
                own_copy(1, term, near_end).wait_send()
                relay_copy(0, other_mid, term, near_end).wait_send()
                relay_copy(2, far_end, term, near_end).wait_send()

        remote(back, back_landed, back_sems.at[0], back_sems.at[1], near_end).wait_send()

    @pl.when(is_end)
    def _():
        @pl.loop(0, terms)
        def _(term):
            own_copy(0, term, near_mid).wait_send()

        @pl.loop(0, moved)
        def _(term):
            end_copy(term).wait_send()


def line_apply(sectors, dims, state, right, combined):
    terms, width, cols = right.shape
    rows = state.shape[0]
    moved = max(1, (terms * 3) // 16)
    tall = combined.shape[1]
    dma = pltpu.SemaphoreType.DMA
    any_space = pl.BlockSpec(memory_space=pl.ANY)
    return pl.pallas_call(
        functools.partial(line_kernel, sectors, moved),
        out_shape=jax.ShapeDtypeStruct((rows, width), F32),
        in_specs=[pl.BlockSpec(memory_space=pltpu.SMEM), any_space, any_space, any_space],
        out_specs=pl.BlockSpec(memory_space=pltpu.VMEM),
        scratch_shapes=[
            pltpu.VMEM((4, rows, width), BF16),
            pltpu.VMEM((width, width), BF16),
            pltpu.VMEM((4, terms, width, cols), BF16),
            pltpu.VMEM((terms, tall, width), BF16),
            pltpu.VMEM((moved, tall, width), BF16),
            pltpu.VMEM((4, tall, cols), F32),
            pltpu.VMEM((4, tall, cols), F32),
            pltpu.VMEM((4, 4, rows, cols), BF16),
            pltpu.VMEM((4, 4, rows, cols), BF16),
            pltpu.VMEM((4, 4, rows, cols), BF16),
            pltpu.VMEM((4, 4, rows, cols), BF16),
            pltpu.VMEM((4, rows, cols), BF16),
            pltpu.VMEM((4, rows, cols), BF16),
            dma((3,)), dma((4,)), dma((4,)),
            dma((2, terms)), dma((3, terms)), dma((4, terms)),
            dma((moved,)), dma((moved,)),
            dma((4, 4)), dma((4, 4)), dma((4,)), dma((4,)), dma((2,)),
        ],
        compiler_params=pltpu.CompilerParams(
            has_side_effects=True, vmem_limit_bytes=56 * 2**20
        ),
    )(dims, state, right, combined)


def passed_along(value, axis, steps):
    count = lax.axis_size(axis)
    first, last = (max(0, -steps), min(count, count - steps))
    return lax.ppermute(value, axis, [(source, source + steps) for source in range(first, last)])


def gathered_apply(sector, live_dim, wave, right, combined, rows, slots):
    width = wave.shape[1]
    terms = right.shape[0]
    whole_state = lax.all_gather(wave, "pan", axis=0, tiled=True)
    indices = lax.iota(jnp.int32, width)
    inside = (indices[:, None] < live_dim) & (indices[None, :] < live_dim)
    masked = jnp.where(inside, whole_state, jnp.zeros((), BF16))
    right_full = lax.all_gather(right, "pan", axis=2, tiled=True)
    term_full = jnp.einsum("ik,wkq->wiq", masked, right_full, preferred_element_type=F32).astype(BF16)
    parts = jnp.einsum(
        "wjri,wiq->jrq", combined.reshape(terms, slots, rows, width), term_full,
        preferred_element_type=F32,
    )
    collected = parts[2]
    for offset in OFFSETS:
        collected = collected + passed_along(parts[offset + 2], "sec", offset)
    return collected


def on_device(
    wave_state, right_blocks, left_blocks, coupling, channel_term, channel_out, sector_dims
):
    rows, width = wave_state.shape[1:]
    terms = right_blocks.shape[1]
    slots = 5
    sector = lax.axis_index("sec")
    live_dim = sector_dims[0]
    cells = channel_term * slots + channel_out - sector + 2
    combined = combine(cells, coupling.astype(F32), left_blocks, terms * slots)
    if lax.axis_size("pan") == 4 and right_blocks.shape[3] % 128 == 0:
        collected = line_apply(
            lax.axis_size("sec"), sector_dims, wave_state[0], right_blocks[0],
            combined.reshape(terms, slots * rows, width),
        )
    else:
        collected = gathered_apply(
            sector, live_dim, wave_state[0], right_blocks[0], combined, rows, slots
        )
    indices = lax.iota(jnp.int32, width)
    row_ids = lax.axis_index("pan") * rows + lax.iota(jnp.int32, rows)
    kept_mask = (row_ids[:, None] < live_dim) & (indices[None, :] < live_dim)
    return jnp.where(kept_mask, collected, jnp.zeros((), F32))[None]


def solution(mesh):
    return jax.shard_map(
        on_device,
        mesh=mesh,
        in_specs=(
            P("sec", "pan", None),
            P("sec", None, None, "pan"),
            P("sec", "pan", None),
            P("sec"),
            P("sec"),
            P("sec"),
            P("sec"),
        ),
        out_specs=P("sec", "pan", None),
        check_vma=False,
    )
```

```python
import functools

import jax
import jax.numpy as jnp
from jax import lax
from jax.experimental import pallas as pl
from jax.experimental.pallas import tpu as pltpu
from jax.sharding import PartitionSpec as P

OFFSETS = (-2, -1, 1, 2)
F32 = jnp.float32
BF16 = jnp.bfloat16


def combine_kernel(cell_ref, coef_ref, left_ref, out_ref, acc_ref):
    acc_ref[...] = jnp.zeros_like(acc_ref)

    @pl.loop(0, left_ref.shape[0])
    def _(channel):
        cell = cell_ref[channel]
        acc_ref[cell] += left_ref[channel].astype(F32) * coef_ref[channel]

    @pl.loop(0, out_ref.shape[0])
    def _(cell):
        out_ref[cell] = acc_ref[cell].astype(BF16)


def combine(cells, coefs, left_blocks, cell_count):
    channels, rows, width = left_blocks.shape
    step = min(rows, 32)
    return pl.pallas_call(
        combine_kernel,
        grid=(rows // step,),
        in_specs=[
            pl.BlockSpec(memory_space=pltpu.SMEM),
            pl.BlockSpec(memory_space=pltpu.SMEM),
            pl.BlockSpec((channels, step, width), lambda i: (0, i, 0)),
        ],
        out_specs=pl.BlockSpec((cell_count, step, width), lambda i: (0, i, 0)),
        out_shape=jax.ShapeDtypeStruct((cell_count, rows, width), BF16),
        scratch_shapes=[pltpu.VMEM((cell_count, step, width), F32)],
        compiler_params=pltpu.CompilerParams(vmem_limit_bytes=48 * 2**20),
        cost_estimate=pl.CostEstimate(
            flops=2 * left_blocks.size, transcendentals=0,
            bytes_accessed=10 * (left_blocks.size + cell_count * rows * width),
        ),
    )(cells, coefs, left_blocks)


def line_kernel(
    sectors, moved, early, dims_ref, state_ref, right_ref, below_ref, above_ref, comb_ref, out_ref,
    state_all, masked, gathered, comb, comb_end, acc, acc_end,
    stage, landed, stage_end, landed_end, back, back_landed,
    local_sems, state_send, state_recv, own_send, relay_send, right_recv,
    end_send, end_recv, part_send, part_recv, part_end_send, part_end_recv, back_sems,
):
    terms, width, cols = right_ref.shape
    rows = state_ref.shape[0]
    me = lax.axis_index("pan")
    sector = lax.axis_index("sec")
    is_mid = (me == 1) | (me == 2)
    is_end = jnp.logical_not(is_mid)
    near_end = jnp.where(me <= 1, 0, 3)
    other_mid = jnp.where(me <= 1, 2, 1)
    far_end = 3 - near_end
    near_mid = jnp.where(me <= 1, 1, 2)

    def remote(src, dst, send, recv, where, axis="pan"):
        return pltpu.make_async_remote_copy(
            src_ref=src, dst_ref=dst, send_sem=send, recv_sem=recv,
            device_id={axis: where}, device_id_type=pl.DeviceIdType.MESH,
        )

    def state_copy(shift):
        where = lax.rem(me + shift, 4)
        spot = state_all.at[me]
        return remote(state_ref, spot, state_send.at[shift], state_recv.at[me], where)

    def state_wait(owner):
        remote(state_ref, state_all.at[owner], state_send.at[0], state_recv.at[owner], me).wait_recv()

    def own_copy(way, term, where):
        return remote(
            right_ref.at[term], gathered.at[me, term],
            own_send.at[way, term], right_recv.at[me, term], where,
        )

    def relay_copy(way, owner, term, where):
        block = gathered.at[owner, term]
        return remote(block, block, relay_send.at[way, term], right_recv.at[owner, term], where)

    def end_copy(term):
        return remote(comb_ref.at[term], comb_end.at[term], end_send.at[term], end_recv.at[term], near_mid)

    def arrived(owner, term):
        block = gathered.at[owner, term]
        remote(block, block, relay_send.at[0, term], right_recv.at[owner, term], me).wait_recv()

    def part_copy(index, owner):
        return remote(
            stage.at[index, owner], landed.at[index, owner],
            part_send.at[index, owner], part_recv.at[index, owner], sector + OFFSETS[index], "sec",
        )

    def part_end_copy(index):
        return remote(
            stage_end.at[index], landed_end.at[index],
            part_end_send.at[index], part_end_recv.at[index], sector + OFFSETS[index], "sec",
        )

    def goes(index):
        target = sector + OFFSETS[index]
        return (target >= 0) & (target < sectors)

    def comes(index):
        source = sector - OFFSETS[index]
        return (source >= 0) & (source < sectors)

    def term_of(step):
        return lax.rem(step + moved, terms)

    for shift in (1, 2, 3):
        state_copy(shift).start()

    @pl.when(is_mid)
    def _():
        @pl.loop(early, terms)
        def _(step):
            own_copy(0, term_of(step), other_mid).start()

            @pl.when(step < terms - moved)
            def _():
                own_copy(1, term_of(step), near_end).start()

    @pl.when(is_end)
    def _():
        @pl.loop(early, terms)
        def _(step):
            own_copy(0, term_of(step), near_mid).start()

        @pl.loop(0, moved)
        def _(term):
            end_copy(term).start()

    copies = [
        pltpu.make_async_copy(state_ref, state_all.at[me], local_sems.at[0]),
        pltpu.make_async_copy(right_ref, gathered.at[me], local_sems.at[1]),
        pltpu.make_async_copy(comb_ref, comb, local_sems.at[2]),
    ]
    spread = pl.ds(moved, early)
    below = pltpu.make_async_copy(
        below_ref, gathered.at[jnp.maximum(me - 1, 0), spread], local_sems.at[3]
    )
    above = pltpu.make_async_copy(
        above_ref, gathered.at[jnp.minimum(me + 1, 3), spread], local_sems.at[4]
    )

    @pl.when(me > 0)
    def _():
        below.start()

    @pl.when(me < 3)
    def _():
        above.start()

    for copy in copies:
        copy.start()
    acc[...] = jnp.zeros_like(acc)
    acc_end[...] = jnp.zeros_like(acc_end)
    for copy in copies:
        copy.wait()

    @pl.when(me > 0)
    def _():
        below.wait()

    @pl.when(me < 3)
    def _():
        above.wait()

    for shift in (1, 2, 3):
        state_wait(lax.rem(me + shift, 4))
    live = dims_ref[0]
    inside_col = lax.broadcasted_iota(jnp.int32, (rows, width), 1) < live
    for owner in range(4):
        row = lax.broadcasted_iota(jnp.int32, (rows, width), 0) + owner * rows
        masked[owner * rows:(owner + 1) * rows, :] = jnp.where(
            inside_col & (row < live), state_all[owner].astype(F32), 0.0
        ).astype(BF16)

    def multiply(owner, term, left, total):
        block = jnp.dot(masked[...], gathered[owner, term], preferred_element_type=F32).astype(BF16)
        total[owner] += jnp.dot(left[term], block, preferred_element_type=F32)

    def send_parts(owner):
        for index in range(4):
            slot = OFFSETS[index] + 2

            @pl.when(goes(index))
            def _():
                stage[index, owner] = acc[owner, slot * rows:(slot + 1) * rows, :].astype(BF16)
                part_copy(index, owner).start()

    @pl.when(is_mid)
    def _():
        @pl.loop(0, terms)
        def _(step):
            term = term_of(step)

            @pl.when(step >= early)
            def _():
                arrived(other_mid, term)

            @pl.when(step < terms - moved)
            def _():
                relay_copy(0, other_mid, term, near_end).start()

            @pl.when(step >= early)
            def _():
                arrived(near_end, term)

            relay_copy(1, near_end, term, other_mid).start()

            @pl.loop(0, 3)
            def _(which):
                owner = jnp.where(which == 0, me, jnp.where(which == 1, other_mid, near_end))
                multiply(owner, term, comb, acc)

        @pl.loop(0, 3)
        def _(which):
            send_parts(jnp.where(which == 0, me, jnp.where(which == 1, other_mid, near_end)))

        @pl.loop(0, terms)
        def _(step):
            term = term_of(step)
            arrived(far_end, term)

            @pl.when(step < terms - moved)
            def _():
                relay_copy(2, far_end, term, near_end).start()

            multiply(far_end, term, comb, acc)

        send_parts(far_end)

        @pl.loop(0, moved)
        def _(term):
            remote(comb_ref.at[term], comb_end.at[term], end_send.at[term], end_recv.at[term], me).wait_recv()

            @pl.loop(0, 4)
            def _(owner):
                multiply(owner, term, comb_end, acc_end)

        for index in range(4):
            slot = OFFSETS[index] + 2

            @pl.when(goes(index))
            def _():
                stage_end[index] = acc_end[:, slot * rows:(slot + 1) * rows, :].astype(BF16)
                part_end_copy(index).start()

        for index in range(4):
            @pl.when(comes(index))
            def _():
                part_end_copy(index).wait_recv()
                acc_end[:, 2 * rows:3 * rows, :] += landed_end[index].astype(F32)

        back[...] = acc_end[:, 2 * rows:3 * rows, :].astype(BF16)
        remote(back, back_landed, back_sems.at[0], back_sems.at[1], near_end).start()

    @pl.when(is_end)
    def _():
        turn = jnp.where(me == 0, 1, -1)

        @pl.loop(0, 4)
        def _(rank):
            owner = me + turn * rank

            @pl.loop(moved, terms)
            def _(term):
                @pl.when((rank > 1) | ((rank == 1) & (term >= moved + early)))
                def _():
                    arrived(owner, term)

                multiply(owner, term, comb, acc)

            send_parts(owner)

    for index in range(4):
        @pl.when(comes(index))
        def _():
            @pl.loop(0, 4)
            def _(owner):
                part_copy(index, owner).wait_recv()
                acc[owner, 2 * rows:3 * rows, :] += landed[index, owner].astype(F32)

    @pl.when(is_end)
    def _():
        remote(back, back_landed, back_sems.at[0], back_sems.at[1], me).wait_recv()
        acc[:, 2 * rows:3 * rows, :] += back_landed[...].astype(F32)

    for owner in range(4):
        out_ref[:, owner * cols:(owner + 1) * cols] = acc[owner, 2 * rows:3 * rows, :]

    for shift in (1, 2, 3):
        state_copy(shift).wait_send()
    for index in range(4):
        @pl.when(goes(index))
        def _():
            @pl.loop(0, 4)
            def _(owner):
                part_copy(index, owner).wait_send()

            @pl.when(is_mid)
            def _():
                part_end_copy(index).wait_send()

    @pl.when(is_mid)
    def _():
        @pl.loop(0, terms)
        def _(step):
            term = term_of(step)
            relay_copy(1, near_end, term, other_mid).wait_send()

            @pl.when(step >= early)
            def _():
                own_copy(0, term, other_mid).wait_send()

            @pl.when((step >= early) & (step < terms - moved))
            def _():
                own_copy(1, term, near_end).wait_send()

            @pl.when(step < terms - moved)
            def _():
                relay_copy(0, other_mid, term, near_end).wait_send()
                relay_copy(2, far_end, term, near_end).wait_send()

        remote(back, back_landed, back_sems.at[0], back_sems.at[1], near_end).wait_send()

    @pl.when(is_end)
    def _():
        @pl.loop(early, terms)
        def _(step):
            own_copy(0, term_of(step), near_mid).wait_send()

        @pl.loop(0, moved)
        def _(term):
            end_copy(term).wait_send()


def line_apply(sectors, moved, early, dims, state, right, below, above, combined):
    terms, width, cols = right.shape
    rows = state.shape[0]
    tall = combined.shape[1]
    dma = pltpu.SemaphoreType.DMA
    any_space = pl.BlockSpec(memory_space=pl.ANY)
    return pl.pallas_call(
        functools.partial(line_kernel, sectors, moved, early),
        out_shape=jax.ShapeDtypeStruct((rows, width), F32),
        in_specs=[pl.BlockSpec(memory_space=pltpu.SMEM)] + [any_space] * 5,
        out_specs=pl.BlockSpec(memory_space=pltpu.VMEM),
        scratch_shapes=[
            pltpu.VMEM((4, rows, width), BF16),
            pltpu.VMEM((width, width), BF16),
            pltpu.VMEM((4, terms, width, cols), BF16),
            pltpu.VMEM((terms, tall, width), BF16),
            pltpu.VMEM((moved, tall, width), BF16),
            pltpu.VMEM((4, tall, cols), F32),
            pltpu.VMEM((4, tall, cols), F32),
            pltpu.VMEM((4, 4, rows, cols), BF16),
            pltpu.VMEM((4, 4, rows, cols), BF16),
            pltpu.VMEM((4, 4, rows, cols), BF16),
            pltpu.VMEM((4, 4, rows, cols), BF16),
            pltpu.VMEM((4, rows, cols), BF16),
            pltpu.VMEM((4, rows, cols), BF16),
            dma((5,)), dma((4,)), dma((4,)),
            dma((2, terms)), dma((3, terms)), dma((4, terms)),
            dma((moved,)), dma((moved,)),
            dma((4, 4)), dma((4, 4)), dma((4,)), dma((4,)), dma((2,)),
        ],
        compiler_params=pltpu.CompilerParams(
            has_side_effects=True, vmem_limit_bytes=56 * 2**20
        ),
    )(dims, state, right, below, above, combined)


def passed_along(value, axis, steps):
    count = lax.axis_size(axis)
    first, last = (max(0, -steps), min(count, count - steps))
    return lax.ppermute(value, axis, [(source, source + steps) for source in range(first, last)])


def gathered_apply(sector, live_dim, wave, right, combined, rows, slots):
    width = wave.shape[1]
    terms = right.shape[0]
    whole_state = lax.all_gather(wave, "pan", axis=0, tiled=True)
    indices = lax.iota(jnp.int32, width)
    inside = (indices[:, None] < live_dim) & (indices[None, :] < live_dim)
    masked = jnp.where(inside, whole_state, jnp.zeros((), BF16))
    right_full = lax.all_gather(right, "pan", axis=2, tiled=True)
    term_full = jnp.einsum("ik,wkq->wiq", masked, right_full, preferred_element_type=F32).astype(BF16)
    parts = jnp.einsum(
        "wjri,wiq->jrq", combined.reshape(terms, slots, rows, width), term_full,
        preferred_element_type=F32,
    )
    collected = parts[2]
    for offset in OFFSETS:
        collected = collected + passed_along(parts[offset + 2], "sec", offset)
    return collected


def on_device(
    wave_state, right_blocks, left_blocks, coupling, channel_term, channel_out, sector_dims
):
    rows, width = wave_state.shape[1:]
    terms = right_blocks.shape[1]
    slots = 5
    sector = lax.axis_index("sec")
    live_dim = sector_dims[0]
    cells = channel_term * slots + channel_out - sector + 2
    in_line = lax.axis_size("pan") == 4 and right_blocks.shape[3] % 128 == 0
    if in_line:
        moved, early = max(1, terms * 3 // 16), max(1, terms // 4)
        lead = right_blocks[0, moved:moved + early]
        below = passed_along(lead, "pan", 1)
        above = passed_along(lead, "pan", -1)
    combined = combine(cells, coupling.astype(F32), left_blocks, terms * slots)
    if in_line:
        collected = line_apply(
            lax.axis_size("sec"), moved, early, sector_dims, wave_state[0], right_blocks[0],
            below, above, combined.reshape(terms, slots * rows, width),
        )
    else:
        collected = gathered_apply(
            sector, live_dim, wave_state[0], right_blocks[0], combined, rows, slots
        )
    indices = lax.iota(jnp.int32, width)
    row_ids = lax.axis_index("pan") * rows + lax.iota(jnp.int32, rows)
    kept_mask = (row_ids[:, None] < live_dim) & (indices[None, :] < live_dim)
    return jnp.where(kept_mask, collected, jnp.zeros((), F32))[None]


def solution(mesh):
    return jax.shard_map(
        on_device,
        mesh=mesh,
        in_specs=(
            P("sec", "pan", None),
            P("sec", None, None, "pan"),
            P("sec", "pan", None),
            P("sec"),
            P("sec"),
            P("sec"),
            P("sec"),
        ),
        out_specs=P("sec", "pan", None),
        check_vma=False,
    )
```

```python
import functools

import jax
import jax.numpy as jnp
from jax import lax
from jax.experimental import pallas as pl
from jax.experimental.pallas import tpu as pltpu
from jax.sharding import PartitionSpec as P

OFFSETS = (-2, -1, 1, 2)
F32 = jnp.float32
BF16 = jnp.bfloat16


def combine_kernel(cell_ref, coef_ref, left_ref, out_ref, acc_ref):
    acc_ref[...] = jnp.zeros_like(acc_ref)

    @pl.loop(0, left_ref.shape[0])
    def _(channel):
        cell = cell_ref[channel]
        acc_ref[cell] += left_ref[channel].astype(F32) * coef_ref[channel]

    @pl.loop(0, out_ref.shape[0])
    def _(cell):
        out_ref[cell] = acc_ref[cell].astype(BF16)


def combine(cells, coefs, left_blocks, cell_count):
    channels, rows, width = left_blocks.shape
    step = min(rows, 32)
    return pl.pallas_call(
        combine_kernel,
        grid=(rows // step,),
        in_specs=[
            pl.BlockSpec(memory_space=pltpu.SMEM),
            pl.BlockSpec(memory_space=pltpu.SMEM),
            pl.BlockSpec((channels, step, width), lambda i: (0, i, 0)),
        ],
        out_specs=pl.BlockSpec((cell_count, step, width), lambda i: (0, i, 0)),
        out_shape=jax.ShapeDtypeStruct((cell_count, rows, width), BF16),
        scratch_shapes=[pltpu.VMEM((cell_count, step, width), F32)],
        compiler_params=pltpu.CompilerParams(vmem_limit_bytes=48 * 2**20),
    )(cells, coefs, left_blocks)


def order_kernel(slots, term_ref, out_ids_ref, coef_ref, table_ref, sorted_ref, spots):
    channels = term_ref.shape[0]
    cells = spots.shape[0]
    last_at, filled_at = 2 * channels, 2 * channels + cells
    sector = lax.axis_index("sec")

    def cell_of(channel):
        return term_ref[channel] * slots + out_ids_ref[channel] - sector + 2

    @pl.loop(0, cells)
    def _(cell):
        spots[cell] = 0

    @pl.loop(0, channels)
    def _(channel):
        spots[cell_of(channel)] += 1

    def lay_out(cell, start):
        count = spots[cell]
        spots[cell] = start
        table_ref[last_at + cell] = jnp.maximum(start + count - 1, 0)
        table_ref[filled_at + cell] = jnp.minimum(count, 1)
        return start + count

    lax.fori_loop(0, cells, lay_out, 0)

    @pl.loop(0, channels)
    def _(channel):
        table_ref[channels + channel] = 1

    @pl.loop(0, cells)
    def _(cell):
        table_ref[channels + jnp.minimum(spots[cell], channels - 1)] = jnp.where(
            table_ref[filled_at + cell] > 0,
            0,
            table_ref[channels + jnp.minimum(spots[cell], channels - 1)],
        )

    @pl.loop(0, channels)
    def _(channel):
        cell = cell_of(channel)
        spot = spots[cell]
        spots[cell] = spot + 1
        table_ref[spot] = channel
        sorted_ref[spot] = coef_ref[channel]


def order_channels(slots, cells, channel_term, channel_out, coefs):
    channels = coefs.shape[0]
    smem = pl.BlockSpec(memory_space=pltpu.SMEM)
    return pl.pallas_call(
        functools.partial(order_kernel, slots),
        out_shape=(
            jax.ShapeDtypeStruct((2 * channels + 2 * cells,), jnp.int32),
            jax.ShapeDtypeStruct((channels,), F32),
        ),
        in_specs=[smem] * 3,
        out_specs=(smem, smem),
        scratch_shapes=[pltpu.SMEM((cells,), jnp.int32)],
    )(channel_term, channel_out, coefs)


def line_kernel(
    sectors, moved, dims_ref, table_ref, coef_ref, state_ref, right_ref, left_ref, out_ref,
    left_all, running, summed,
    state_all, masked, gathered, comb, comb_end, acc, acc_end,
    stage, landed, stage_end, landed_end, back, back_landed,
    local_sems, state_send, state_recv, own_send, relay_send, right_recv,
    end_send, end_recv, part_send, part_recv, part_end_send, part_end_recv, back_sems,
):
    terms, width, cols = right_ref.shape
    rows = state_ref.shape[0]
    slots = comb.shape[1] // rows
    me = lax.axis_index("pan")
    sector = lax.axis_index("sec")
    is_mid = (me == 1) | (me == 2)
    is_end = jnp.logical_not(is_mid)
    near_end = jnp.where(me <= 1, 0, 3)
    other_mid = jnp.where(me <= 1, 2, 1)
    far_end = 3 - near_end
    near_mid = jnp.where(me <= 1, 1, 2)

    def remote(src, dst, send, recv, where, axis="pan"):
        return pltpu.make_async_remote_copy(
            src_ref=src, dst_ref=dst, send_sem=send, recv_sem=recv,
            device_id={axis: where}, device_id_type=pl.DeviceIdType.MESH,
        )

    def state_copy(shift):
        where = lax.rem(me + shift, 4)
        spot = state_all.at[me]
        return remote(state_ref, spot, state_send.at[shift], state_recv.at[me], where)

    def state_wait(owner):
        remote(state_ref, state_all.at[owner], state_send.at[0], state_recv.at[owner], me).wait_recv()

    def own_copy(way, term, where):
        return remote(
            right_ref.at[term], gathered.at[me, term],
            own_send.at[way, term], right_recv.at[me, term], where,
        )

    def relay_copy(way, owner, term, where):
        block = gathered.at[owner, term]
        return remote(block, block, relay_send.at[way, term], right_recv.at[owner, term], where)

    def end_copy(term):
        return remote(comb.at[term], comb_end.at[term], end_send.at[term], end_recv.at[term], near_mid)

    def arrived(owner, term):
        block = gathered.at[owner, term]
        remote(block, block, relay_send.at[0, term], right_recv.at[owner, term], me).wait_recv()

    def part_copy(index, owner):
        return remote(
            stage.at[index, owner], landed.at[index, owner],
            part_send.at[index, owner], part_recv.at[index, owner], sector + OFFSETS[index], "sec",
        )

    def part_end_copy(index):
        return remote(
            stage_end.at[index], landed_end.at[index],
            part_end_send.at[index], part_end_recv.at[index], sector + OFFSETS[index], "sec",
        )

    def goes(index):
        target = sector + OFFSETS[index]
        return (target >= 0) & (target < sectors)

    def comes(index):
        source = sector - OFFSETS[index]
        return (source >= 0) & (source < sectors)

    for shift in (1, 2, 3):
        state_copy(shift).start()

    @pl.when(is_mid)
    def _():
        @pl.loop(0, terms)
        def _(term):
            own_copy(0, term, other_mid).start()

            @pl.when(term >= moved)
            def _():
                own_copy(1, term, near_end).start()

    @pl.when(is_end)
    def _():
        @pl.loop(0, terms)
        def _(term):
            own_copy(0, term, near_mid).start()

    copies = [
        pltpu.make_async_copy(state_ref, state_all.at[me], local_sems.at[0]),
        pltpu.make_async_copy(right_ref, gathered.at[me], local_sems.at[1]),
        pltpu.make_async_copy(left_ref, left_all, local_sems.at[2]),
    ]
    for copy in copies:
        copy.start()
    acc[...] = jnp.zeros_like(acc)
    acc_end[...] = jnp.zeros_like(acc_end)
    running[...] = jnp.zeros_like(running)
    for copy in copies:
        copy.wait()

    channels = left_all.shape[0]
    cells = terms * slots

    @pl.loop(0, channels)
    def _(step):
        kept = table_ref[channels + step].astype(F32)
        total = running[...] * kept + left_all[table_ref[step]].astype(F32) * coef_ref[step]
        running[...] = total
        summed[step] = total.astype(BF16)

    @pl.loop(0, terms)
    def _(term):
        for slot in range(slots):
            cell = term * slots + slot
            filled = table_ref[2 * channels + cells + cell].astype(F32)
            value = summed[table_ref[2 * channels + cell]].astype(F32) * filled
            comb[term, slot * rows:(slot + 1) * rows, :] = value.astype(BF16)

    for shift in (1, 2, 3):
        state_wait(lax.rem(me + shift, 4))

    @pl.when(is_end)
    def _():
        @pl.loop(0, moved)
        def _(term):
            end_copy(term).start()

    live = dims_ref[0]
    inside_col = lax.broadcasted_iota(jnp.int32, (rows, width), 1) < live
    for owner in range(4):
        row = lax.broadcasted_iota(jnp.int32, (rows, width), 0) + owner * rows
        masked[owner * rows:(owner + 1) * rows, :] = jnp.where(
            inside_col & (row < live), state_all[owner].astype(F32), 0.0
        ).astype(BF16)

    def multiply(owner, term, left, total):
        block = jnp.dot(masked[...], gathered[owner, term], preferred_element_type=F32).astype(BF16)
        total[owner] += jnp.dot(left[term], block, preferred_element_type=F32)

    def send_parts(owner):
        for index in range(4):
            slot = OFFSETS[index] + 2

            @pl.when(goes(index))
            def _():
                stage[index, owner] = acc[owner, slot * rows:(slot + 1) * rows, :].astype(BF16)
                part_copy(index, owner).start()

    @pl.when(is_mid)
    def _():
        @pl.loop(0, terms)
        def _(term):
            arrived(other_mid, term)

            @pl.when(term >= moved)
            def _():
                relay_copy(0, other_mid, term, near_end).start()

            arrived(near_end, term)
            relay_copy(1, near_end, term, other_mid).start()

            @pl.loop(0, 3)
            def _(which):
                owner = jnp.where(which == 0, me, jnp.where(which == 1, other_mid, near_end))
                multiply(owner, term, comb, acc)

        @pl.loop(0, 3)
        def _(which):
            send_parts(jnp.where(which == 0, me, jnp.where(which == 1, other_mid, near_end)))

        @pl.loop(0, terms)
        def _(term):
            arrived(far_end, term)

            @pl.when(term >= moved)
            def _():
                relay_copy(2, far_end, term, near_end).start()

            multiply(far_end, term, comb, acc)

        send_parts(far_end)

        @pl.loop(0, moved)
        def _(term):
            remote(comb.at[term], comb_end.at[term], end_send.at[term], end_recv.at[term], me).wait_recv()

            @pl.loop(0, 4)
            def _(owner):
                multiply(owner, term, comb_end, acc_end)

        for index in range(4):
            slot = OFFSETS[index] + 2

            @pl.when(goes(index))
            def _():
                stage_end[index] = acc_end[:, slot * rows:(slot + 1) * rows, :].astype(BF16)
                part_end_copy(index).start()

        for index in range(4):
            @pl.when(comes(index))
            def _():
                part_end_copy(index).wait_recv()
                acc_end[:, 2 * rows:3 * rows, :] += landed_end[index].astype(F32)

        back[...] = acc_end[:, 2 * rows:3 * rows, :].astype(BF16)
        remote(back, back_landed, back_sems.at[0], back_sems.at[1], near_end).start()

    @pl.when(is_end)
    def _():
        turn = jnp.where(me == 0, 1, -1)

        @pl.loop(0, 4)
        def _(rank):
            owner = me + turn * rank

            @pl.loop(moved, terms)
            def _(term):
                @pl.when(rank > 0)
                def _():
                    arrived(owner, term)

                multiply(owner, term, comb, acc)

            send_parts(owner)

    for index in range(4):
        @pl.when(comes(index))
        def _():
            @pl.loop(0, 4)
            def _(owner):
                part_copy(index, owner).wait_recv()
                acc[owner, 2 * rows:3 * rows, :] += landed[index, owner].astype(F32)

    @pl.when(is_end)
    def _():
        remote(back, back_landed, back_sems.at[0], back_sems.at[1], me).wait_recv()
        acc[:, 2 * rows:3 * rows, :] += back_landed[...].astype(F32)

    for owner in range(4):
        out_ref[:, owner * cols:(owner + 1) * cols] = acc[owner, 2 * rows:3 * rows, :]

    for shift in (1, 2, 3):
        state_copy(shift).wait_send()
    for index in range(4):
        @pl.when(goes(index))
        def _():
            @pl.loop(0, 4)
            def _(owner):
                part_copy(index, owner).wait_send()

            @pl.when(is_mid)
            def _():
                part_end_copy(index).wait_send()

    @pl.when(is_mid)
    def _():
        @pl.loop(0, terms)
        def _(term):
            own_copy(0, term, other_mid).wait_send()
            relay_copy(1, near_end, term, other_mid).wait_send()

            @pl.when(term >= moved)
            def _():
                own_copy(1, term, near_end).wait_send()
                relay_copy(0, other_mid, term, near_end).wait_send()
                relay_copy(2, far_end, term, near_end).wait_send()

        remote(back, back_landed, back_sems.at[0], back_sems.at[1], near_end).wait_send()

    @pl.when(is_end)
    def _():
        @pl.loop(0, terms)
        def _(term):
            own_copy(0, term, near_mid).wait_send()

        @pl.loop(0, moved)
        def _(term):
            end_copy(term).wait_send()


def line_apply(sectors, slots, dims, table, coefs, state, right, left):
    terms, width, cols = right.shape
    rows = state.shape[0]
    moved = max(1, (terms * 3) // 16)
    tall = slots * rows
    dma = pltpu.SemaphoreType.DMA
    any_space = pl.BlockSpec(memory_space=pl.ANY)
    return pl.pallas_call(
        functools.partial(line_kernel, sectors, moved),
        out_shape=jax.ShapeDtypeStruct((rows, width), F32),
        in_specs=[pl.BlockSpec(memory_space=pltpu.SMEM)] * 3 + [any_space] * 3,
        out_specs=pl.BlockSpec(memory_space=pltpu.VMEM),
        scratch_shapes=[
            pltpu.VMEM(left.shape, BF16),
            pltpu.VMEM((rows, width), F32),
            pltpu.VMEM(left.shape, BF16),
            pltpu.VMEM((4, rows, width), BF16),
            pltpu.VMEM((width, width), BF16),
            pltpu.VMEM((4, terms, width, cols), BF16),
            pltpu.VMEM((terms, tall, width), BF16),
            pltpu.VMEM((moved, tall, width), BF16),
            pltpu.VMEM((4, tall, cols), F32),
            pltpu.VMEM((4, tall, cols), F32),
            pltpu.VMEM((4, 4, rows, cols), BF16),
            pltpu.VMEM((4, 4, rows, cols), BF16),
            pltpu.VMEM((4, 4, rows, cols), BF16),
            pltpu.VMEM((4, 4, rows, cols), BF16),
            pltpu.VMEM((4, rows, cols), BF16),
            pltpu.VMEM((4, rows, cols), BF16),
            dma((3,)), dma((4,)), dma((4,)),
            dma((2, terms)), dma((3, terms)), dma((4, terms)),
            dma((moved,)), dma((moved,)),
            dma((4, 4)), dma((4, 4)), dma((4,)), dma((4,)), dma((2,)),
        ],
        compiler_params=pltpu.CompilerParams(
            has_side_effects=True, vmem_limit_bytes=56 * 2**20
        ),
    )(dims, table, coefs, state, right, left)


def passed_along(value, axis, steps):
    count = lax.axis_size(axis)
    first, last = (max(0, -steps), min(count, count - steps))
    return lax.ppermute(value, axis, [(source, source + steps) for source in range(first, last)])


def gathered_apply(sector, live_dim, wave, right, combined, rows, slots):
    width = wave.shape[1]
    terms = right.shape[0]
    whole_state = lax.all_gather(wave, "pan", axis=0, tiled=True)
    indices = lax.iota(jnp.int32, width)
    inside = (indices[:, None] < live_dim) & (indices[None, :] < live_dim)
    masked = jnp.where(inside, whole_state, jnp.zeros((), BF16))
    right_full = lax.all_gather(right, "pan", axis=2, tiled=True)
    term_full = jnp.einsum("ik,wkq->wiq", masked, right_full, preferred_element_type=F32).astype(BF16)
    parts = jnp.einsum(
        "wjri,wiq->jrq", combined.reshape(terms, slots, rows, width), term_full,
        preferred_element_type=F32,
    )
    collected = parts[2]
    for offset in OFFSETS:
        collected = collected + passed_along(parts[offset + 2], "sec", offset)
    return collected


def on_device(
    wave_state, right_blocks, left_blocks, coupling, channel_term, channel_out, sector_dims
):
    rows, width = wave_state.shape[1:]
    terms = right_blocks.shape[1]
    slots = 5
    sector = lax.axis_index("sec")
    live_dim = sector_dims[0]
    cells = channel_term * slots + channel_out - sector + 2
    coefs = coupling.astype(F32)
    if lax.axis_size("pan") == 4 and right_blocks.shape[3] % 128 == 0:
        table, ordered = order_channels(slots, terms * slots, channel_term, channel_out, coefs)
        collected = line_apply(
            lax.axis_size("sec"), slots, sector_dims, table, ordered,
            wave_state[0], right_blocks[0], left_blocks,
        )
    else:
        combined = combine(cells, coefs, left_blocks, terms * slots)
        collected = gathered_apply(
            sector, live_dim, wave_state[0], right_blocks[0], combined, rows, slots
        )
    indices = lax.iota(jnp.int32, width)
    row_ids = lax.axis_index("pan") * rows + lax.iota(jnp.int32, rows)
    kept_mask = (row_ids[:, None] < live_dim) & (indices[None, :] < live_dim)
    return jnp.where(kept_mask, collected, jnp.zeros((), F32))[None]


def solution(mesh):
    return jax.shard_map(
        on_device,
        mesh=mesh,
        in_specs=(
            P("sec", "pan", None),
            P("sec", None, None, "pan"),
            P("sec", "pan", None),
            P("sec"),
            P("sec"),
            P("sec"),
            P("sec"),
        ),
        out_specs=P("sec", "pan", None),
        check_vma=False,
    )
```

```python
import functools

import jax
import jax.numpy as jnp
from jax import lax
from jax.experimental import pallas as pl
from jax.experimental.pallas import tpu as pltpu
from jax.sharding import PartitionSpec as P

OFFSETS = (-2, -1, 1, 2)
F32 = jnp.float32
BF16 = jnp.bfloat16


def combine_kernel(cell_ref, coef_ref, left_ref, out_ref, acc_ref):
    acc_ref[...] = jnp.zeros_like(acc_ref)

    @pl.loop(0, left_ref.shape[0])
    def _(channel):
        cell = cell_ref[channel]
        acc_ref[cell] += left_ref[channel].astype(F32) * coef_ref[channel]

    @pl.loop(0, out_ref.shape[0])
    def _(cell):
        out_ref[cell] = acc_ref[cell].astype(BF16)


def combine(cells, coefs, left_blocks, cell_count):
    channels, rows, width = left_blocks.shape
    step = min(rows, 32)
    return pl.pallas_call(
        combine_kernel,
        grid=(rows // step,),
        in_specs=[
            pl.BlockSpec(memory_space=pltpu.SMEM),
            pl.BlockSpec(memory_space=pltpu.SMEM),
            pl.BlockSpec((channels, step, width), lambda i: (0, i, 0)),
        ],
        out_specs=pl.BlockSpec((cell_count, step, width), lambda i: (0, i, 0)),
        out_shape=jax.ShapeDtypeStruct((cell_count, rows, width), BF16),
        scratch_shapes=[pltpu.VMEM((cell_count, step, width), F32)],
        compiler_params=pltpu.CompilerParams(vmem_limit_bytes=48 * 2**20),
    )(cells, coefs, left_blocks)


def order_kernel(slots, term_ref, out_ids_ref, coef_ref, table_ref, sorted_ref, spots):
    channels = term_ref.shape[0]
    cells = spots.shape[0]
    last_at, filled_at = 2 * channels, 2 * channels + cells
    sector = lax.axis_index("sec")

    def cell_of(channel):
        return term_ref[channel] * slots + out_ids_ref[channel] - sector + 2

    @pl.loop(0, cells)
    def _(cell):
        spots[cell] = 0

    @pl.loop(0, channels)
    def _(channel):
        spots[cell_of(channel)] += 1

    def lay_out(cell, start):
        count = spots[cell]
        spots[cell] = start
        table_ref[last_at + cell] = jnp.maximum(start + count - 1, 0)
        table_ref[filled_at + cell] = jnp.minimum(count, 1)
        return start + count

    lax.fori_loop(0, cells, lay_out, 0)

    @pl.loop(0, channels)
    def _(channel):
        table_ref[channels + channel] = 1

    @pl.loop(0, cells)
    def _(cell):
        table_ref[channels + jnp.minimum(spots[cell], channels - 1)] = jnp.where(
            table_ref[filled_at + cell] > 0,
            0,
            table_ref[channels + jnp.minimum(spots[cell], channels - 1)],
        )

    @pl.loop(0, channels)
    def _(channel):
        cell = cell_of(channel)
        spot = spots[cell]
        spots[cell] = spot + 1
        table_ref[spot] = channel
        sorted_ref[spot] = coef_ref[channel]


def order_channels(slots, cells, channel_term, channel_out, coefs):
    channels = coefs.shape[0]
    smem = pl.BlockSpec(memory_space=pltpu.SMEM)
    return pl.pallas_call(
        functools.partial(order_kernel, slots),
        out_shape=(
            jax.ShapeDtypeStruct((2 * channels + 2 * cells,), jnp.int32),
            jax.ShapeDtypeStruct((channels,), F32),
        ),
        in_specs=[smem] * 3,
        out_specs=(smem, smem),
        scratch_shapes=[pltpu.SMEM((cells,), jnp.int32)],
    )(channel_term, channel_out, coefs)


def line_kernel(
    sectors, moved, dims_ref, table_ref, coef_ref, state_ref, right_ref, left_ref, out_ref,
    left_all, running, summed,
    state_all, masked, gathered, comb, comb_end, acc, acc_end,
    stage, landed, stage_end, landed_end, back, back_landed,
    local_sems, state_send, state_recv, own_send, relay_send, right_recv,
    end_send, end_recv, part_send, part_recv, part_end_send, part_end_recv, back_sems,
):
    terms, width, cols = right_ref.shape
    rows = state_ref.shape[0]
    slots = comb.shape[1] // rows
    me = lax.axis_index("pan")
    sector = lax.axis_index("sec")
    is_mid = (me == 1) | (me == 2)
    is_end = jnp.logical_not(is_mid)
    near_end = jnp.where(me <= 1, 0, 3)
    other_mid = jnp.where(me <= 1, 2, 1)
    far_end = 3 - near_end
    near_mid = jnp.where(me <= 1, 1, 2)

    def remote(src, dst, send, recv, where, axis="pan"):
        return pltpu.make_async_remote_copy(
            src_ref=src, dst_ref=dst, send_sem=send, recv_sem=recv,
            device_id={axis: where}, device_id_type=pl.DeviceIdType.MESH,
        )

    def state_copy(shift):
        where = lax.rem(me + shift, 4)
        spot = state_all.at[me]
        return remote(state_ref, spot, state_send.at[shift], state_recv.at[me], where)

    def state_wait(owner):
        remote(state_ref, state_all.at[owner], state_send.at[0], state_recv.at[owner], me).wait_recv()

    def own_copy(way, term, where):
        return remote(
            right_ref.at[term], gathered.at[me, term],
            own_send.at[way, term], right_recv.at[me, term], where,
        )

    def relay_copy(way, owner, term, where):
        block = gathered.at[owner, term]
        return remote(block, block, relay_send.at[way, term], right_recv.at[owner, term], where)

    def end_copy(term):
        return remote(comb.at[term], comb_end.at[term], end_send.at[term], end_recv.at[term], near_mid)

    def end_copy_arrived(term):
        remote(comb.at[term], comb_end.at[term], end_send.at[term], end_recv.at[term], me).wait_recv()

    def arrived(owner, term):
        block = gathered.at[owner, term]
        remote(block, block, relay_send.at[0, term], right_recv.at[owner, term], me).wait_recv()

    def part_copy(index, owner):
        return remote(
            stage.at[index, owner], landed.at[index, owner],
            part_send.at[index, owner], part_recv.at[index, owner], sector + OFFSETS[index], "sec",
        )

    def part_end_copy(index):
        return remote(
            stage_end.at[index], landed_end.at[index],
            part_end_send.at[index], part_end_recv.at[index], sector + OFFSETS[index], "sec",
        )

    def goes(index):
        target = sector + OFFSETS[index]
        return (target >= 0) & (target < sectors)

    def comes(index):
        source = sector - OFFSETS[index]
        return (source >= 0) & (source < sectors)

    for shift in (1, 2, 3):
        state_copy(shift).start()

    @pl.when(is_mid)
    def _():
        @pl.loop(0, terms)
        def _(term):
            own_copy(0, term, other_mid).start()

            @pl.when(term >= moved)
            def _():
                own_copy(1, term, near_end).start()

    ahead = terms * 3 // 8

    @pl.when(is_end)
    def _():
        @pl.loop(0, ahead)
        def _(term):
            own_copy(0, term, near_mid).start()

    copies = [
        pltpu.make_async_copy(state_ref, state_all.at[me], local_sems.at[0]),
        pltpu.make_async_copy(right_ref, gathered.at[me], local_sems.at[1]),
        pltpu.make_async_copy(left_ref, left_all, local_sems.at[2]),
    ]
    for copy in copies:
        copy.start()
    acc[...] = jnp.zeros_like(acc)
    acc_end[...] = jnp.zeros_like(acc_end)
    running[...] = jnp.zeros_like(running)
    for copy in copies:
        copy.wait()

    channels = left_all.shape[0]
    cells = terms * slots

    @pl.loop(0, channels)
    def _(step):
        kept = table_ref[channels + step].astype(F32)
        total = running[...] * kept + left_all[table_ref[step]].astype(F32) * coef_ref[step]
        running[...] = total
        summed[step] = total.astype(BF16)

    @pl.loop(0, terms)
    def _(term):
        for slot in range(slots):
            cell = term * slots + slot
            filled = table_ref[2 * channels + cells + cell].astype(F32)
            value = summed[table_ref[2 * channels + cell]].astype(F32) * filled
            comb[term, slot * rows:(slot + 1) * rows, :] = value.astype(BF16)

    for shift in (1, 2, 3):
        state_wait(lax.rem(me + shift, 4))

    @pl.when(is_end)
    def _():
        for turn in range(moved):
            left = terms - ahead
            first = ahead + left * turn // moved

            @pl.when(turn < moved - 1)
            def _():
                end_copy(turn).start()

            @pl.loop(first, ahead + left * (turn + 1) // moved)
            def _(term):
                own_copy(0, term, near_mid).start()

        end_copy(moved - 1).start()

    live = dims_ref[0]
    inside_col = lax.broadcasted_iota(jnp.int32, (rows, width), 1) < live
    for owner in range(4):
        row = lax.broadcasted_iota(jnp.int32, (rows, width), 0) + owner * rows
        masked[owner * rows:(owner + 1) * rows, :] = jnp.where(
            inside_col & (row < live), state_all[owner].astype(F32), 0.0
        ).astype(BF16)

    def multiply(owner, term, left, total):
        block = jnp.dot(masked[...], gathered[owner, term], preferred_element_type=F32).astype(BF16)
        total[owner] += jnp.dot(left[term], block, preferred_element_type=F32)

    def send_parts(owner):
        for index in range(4):
            slot = OFFSETS[index] + 2

            @pl.when(goes(index))
            def _():
                stage[index, owner] = acc[owner, slot * rows:(slot + 1) * rows, :].astype(BF16)
                part_copy(index, owner).start()

    end_lag, far_lag, extra_lag = terms * 3 // 8, terms * 11 // 16, terms * 11 // 8

    def extra(term):
        end_copy_arrived(term)

        @pl.loop(0, 4)
        def _(owner):
            multiply(owner, term, comb_end, acc_end)

    @pl.when(is_mid)
    def _():
        @pl.loop(0, terms + far_lag)
        def _(tick):
            near, far, late = tick - end_lag, tick - far_lag, tick - extra_lag

            @pl.when(tick < terms)
            def _():
                arrived(other_mid, tick)

                @pl.when(tick >= moved)
                def _():
                    relay_copy(0, other_mid, tick, near_end).start()

            @pl.when((near >= 0) & (near < terms))
            def _():
                arrived(near_end, near)
                relay_copy(1, near_end, near, other_mid).start()

            @pl.when(far >= 0)
            def _():
                arrived(far_end, far)

                @pl.when(far >= moved)
                def _():
                    relay_copy(2, far_end, far, near_end).start()

            @pl.when(tick < terms)
            def _():
                @pl.loop(0, 2)
                def _(which):
                    multiply(jnp.where(which == 0, me, other_mid), tick, comb, acc)

            @pl.when((near >= 0) & (near < terms))
            def _():
                multiply(near_end, near, comb, acc)

            @pl.when(far >= 0)
            def _():
                multiply(far_end, far, comb, acc)

            @pl.when((late >= 0) & (late < moved - 1))
            def _():
                extra(late)

        @pl.loop(0, 4)
        def _(owner):
            send_parts(owner)

        extra(moved - 1)

        for index in range(4):
            slot = OFFSETS[index] + 2

            @pl.when(goes(index))
            def _():
                stage_end[index] = acc_end[:, slot * rows:(slot + 1) * rows, :].astype(BF16)
                part_end_copy(index).start()

        for index in range(4):
            @pl.when(comes(index))
            def _():
                part_end_copy(index).wait_recv()
                acc_end[:, 2 * rows:3 * rows, :] += landed_end[index].astype(F32)

        back[...] = acc_end[:, 2 * rows:3 * rows, :].astype(BF16)
        remote(back, back_landed, back_sems.at[0], back_sems.at[1], near_end).start()

    @pl.when(is_end)
    def _():
        turn = jnp.where(me == 0, 1, -1)

        @pl.loop(0, 4)
        def _(rank):
            owner = me + turn * rank

            @pl.loop(moved, terms)
            def _(term):
                @pl.when(rank > 0)
                def _():
                    arrived(owner, term)

                multiply(owner, term, comb, acc)

            send_parts(owner)

    for index in range(4):
        @pl.when(comes(index))
        def _():
            @pl.loop(0, 4)
            def _(owner):
                part_copy(index, owner).wait_recv()
                acc[owner, 2 * rows:3 * rows, :] += landed[index, owner].astype(F32)

    @pl.when(is_end)
    def _():
        remote(back, back_landed, back_sems.at[0], back_sems.at[1], me).wait_recv()
        acc[:, 2 * rows:3 * rows, :] += back_landed[...].astype(F32)

    for owner in range(4):
        out_ref[:, owner * cols:(owner + 1) * cols] = acc[owner, 2 * rows:3 * rows, :]

    for shift in (1, 2, 3):
        state_copy(shift).wait_send()
    for index in range(4):
        @pl.when(goes(index))
        def _():
            @pl.loop(0, 4)
            def _(owner):
                part_copy(index, owner).wait_send()

            @pl.when(is_mid)
            def _():
                part_end_copy(index).wait_send()

    @pl.when(is_mid)
    def _():
        @pl.loop(0, terms)
        def _(term):
            own_copy(0, term, other_mid).wait_send()
            relay_copy(1, near_end, term, other_mid).wait_send()

            @pl.when(term >= moved)
            def _():
                own_copy(1, term, near_end).wait_send()
                relay_copy(0, other_mid, term, near_end).wait_send()
                relay_copy(2, far_end, term, near_end).wait_send()

        remote(back, back_landed, back_sems.at[0], back_sems.at[1], near_end).wait_send()

    @pl.when(is_end)
    def _():
        @pl.loop(0, terms)
        def _(term):
            own_copy(0, term, near_mid).wait_send()

        @pl.loop(0, moved)
        def _(term):
            end_copy(term).wait_send()


def line_apply(sectors, slots, dims, table, coefs, state, right, left):
    terms, width, cols = right.shape
    rows = state.shape[0]
    moved = max(1, terms // 4)
    tall = slots * rows
    dma = pltpu.SemaphoreType.DMA
    any_space = pl.BlockSpec(memory_space=pl.ANY)
    return pl.pallas_call(
        functools.partial(line_kernel, sectors, moved),
        out_shape=jax.ShapeDtypeStruct((rows, width), F32),
        in_specs=[pl.BlockSpec(memory_space=pltpu.SMEM)] * 3 + [any_space] * 3,
        out_specs=pl.BlockSpec(memory_space=pltpu.VMEM),
        scratch_shapes=[
            pltpu.VMEM(left.shape, BF16),
            pltpu.VMEM((rows, width), F32),
            pltpu.VMEM(left.shape, BF16),
            pltpu.VMEM((4, rows, width), BF16),
            pltpu.VMEM((width, width), BF16),
            pltpu.VMEM((4, terms, width, cols), BF16),
            pltpu.VMEM((terms, tall, width), BF16),
            pltpu.VMEM((moved, tall, width), BF16),
            pltpu.VMEM((4, tall, cols), F32),
            pltpu.VMEM((4, tall, cols), F32),
            pltpu.VMEM((4, 4, rows, cols), BF16),
            pltpu.VMEM((4, 4, rows, cols), BF16),
            pltpu.VMEM((4, 4, rows, cols), BF16),
            pltpu.VMEM((4, 4, rows, cols), BF16),
            pltpu.VMEM((4, rows, cols), BF16),
            pltpu.VMEM((4, rows, cols), BF16),
            dma((3,)), dma((4,)), dma((4,)),
            dma((2, terms)), dma((3, terms)), dma((4, terms)),
            dma((moved,)), dma((moved,)),
            dma((4, 4)), dma((4, 4)), dma((4,)), dma((4,)), dma((2,)),
        ],
        compiler_params=pltpu.CompilerParams(
            has_side_effects=True, vmem_limit_bytes=56 * 2**20
        ),
    )(dims, table, coefs, state, right, left)


def passed_along(value, axis, steps):
    count = lax.axis_size(axis)
    first, last = (max(0, -steps), min(count, count - steps))
    return lax.ppermute(value, axis, [(source, source + steps) for source in range(first, last)])


def gathered_apply(sector, live_dim, wave, right, combined, rows, slots):
    width = wave.shape[1]
    terms = right.shape[0]
    whole_state = lax.all_gather(wave, "pan", axis=0, tiled=True)
    indices = lax.iota(jnp.int32, width)
    inside = (indices[:, None] < live_dim) & (indices[None, :] < live_dim)
    masked = jnp.where(inside, whole_state, jnp.zeros((), BF16))
    right_full = lax.all_gather(right, "pan", axis=2, tiled=True)
    term_full = jnp.einsum("ik,wkq->wiq", masked, right_full, preferred_element_type=F32).astype(BF16)
    parts = jnp.einsum(
        "wjri,wiq->jrq", combined.reshape(terms, slots, rows, width), term_full,
        preferred_element_type=F32,
    )
    collected = parts[2]
    for offset in OFFSETS:
        collected = collected + passed_along(parts[offset + 2], "sec", offset)
    return collected


def on_device(
    wave_state, right_blocks, left_blocks, coupling, channel_term, channel_out, sector_dims
):
    rows, width = wave_state.shape[1:]
    terms = right_blocks.shape[1]
    slots = 5
    sector = lax.axis_index("sec")
    live_dim = sector_dims[0]
    cells = channel_term * slots + channel_out - sector + 2
    coefs = coupling.astype(F32)
    if lax.axis_size("pan") == 4 and right_blocks.shape[3] % 128 == 0:
        table, ordered = order_channels(slots, terms * slots, channel_term, channel_out, coefs)
        collected = line_apply(
            lax.axis_size("sec"), slots, sector_dims, table, ordered,
            wave_state[0], right_blocks[0], left_blocks,
        )
    else:
        combined = combine(cells, coefs, left_blocks, terms * slots)
        collected = gathered_apply(
            sector, live_dim, wave_state[0], right_blocks[0], combined, rows, slots
        )
    indices = lax.iota(jnp.int32, width)
    row_ids = lax.axis_index("pan") * rows + lax.iota(jnp.int32, rows)
    kept_mask = (row_ids[:, None] < live_dim) & (indices[None, :] < live_dim)
    return jnp.where(kept_mask, collected, jnp.zeros((), F32))[None]


def solution(mesh):
    return jax.shard_map(
        on_device,
        mesh=mesh,
        in_specs=(
            P("sec", "pan", None),
            P("sec", None, None, "pan"),
            P("sec", "pan", None),
            P("sec"),
            P("sec"),
            P("sec"),
            P("sec"),
        ),
        out_specs=P("sec", "pan", None),
        check_vma=False,
    )
```

```python
import functools

import jax
import jax.numpy as jnp
from jax import lax
from jax.experimental import pallas as pl
from jax.experimental.pallas import tpu as pltpu
from jax.sharding import PartitionSpec as P

OFFSETS = (-2, -1, 1, 2)
F32 = jnp.float32
BF16 = jnp.bfloat16


def combine_kernel(cell_ref, coef_ref, left_ref, out_ref, acc_ref):
    acc_ref[...] = jnp.zeros_like(acc_ref)

    @pl.loop(0, left_ref.shape[0])
    def _(channel):
        cell = cell_ref[channel]
        acc_ref[cell] += left_ref[channel].astype(F32) * coef_ref[channel]

    @pl.loop(0, out_ref.shape[0])
    def _(cell):
        out_ref[cell] = acc_ref[cell].astype(BF16)


def combine(cells, coefs, left_blocks, cell_count):
    channels, rows, width = left_blocks.shape
    step = min(rows, 32)
    return pl.pallas_call(
        combine_kernel,
        grid=(rows // step,),
        in_specs=[
            pl.BlockSpec(memory_space=pltpu.SMEM),
            pl.BlockSpec(memory_space=pltpu.SMEM),
            pl.BlockSpec((channels, step, width), lambda i: (0, i, 0)),
        ],
        out_specs=pl.BlockSpec((cell_count, step, width), lambda i: (0, i, 0)),
        out_shape=jax.ShapeDtypeStruct((cell_count, rows, width), BF16),
        scratch_shapes=[pltpu.VMEM((cell_count, step, width), F32)],
        compiler_params=pltpu.CompilerParams(vmem_limit_bytes=48 * 2**20),
    )(cells, coefs, left_blocks)


def order_kernel(slots, term_ref, out_ids_ref, coef_ref, table_ref, sorted_ref, spots):
    channels = term_ref.shape[0]
    cells = spots.shape[0]
    last_at, filled_at = 2 * channels, 2 * channels + cells
    sector = lax.axis_index("sec")

    def cell_of(channel):
        return term_ref[channel] * slots + out_ids_ref[channel] - sector + 2

    @pl.loop(0, cells, unroll=8)
    def _(cell):
        spots[cell] = 0

    @pl.loop(0, channels, unroll=4)
    def _(channel):
        spots[cell_of(channel)] += 1
        table_ref[channels + channel] = 1

    def lay_out(cell, start):
        count = spots[cell]
        spots[cell] = start
        table_ref[last_at + cell] = jnp.maximum(start + count - 1, 0)
        filled = jnp.minimum(count, 1)
        table_ref[filled_at + cell] = filled
        first = channels + jnp.minimum(start, channels - 1)
        table_ref[first] = jnp.where(count > 0, 0, table_ref[first])
        return start + count

    lax.fori_loop(0, cells, lay_out, 0, unroll=4)

    @pl.loop(0, channels, unroll=4)
    def _(channel):
        cell = cell_of(channel)
        spot = spots[cell]
        spots[cell] = spot + 1
        table_ref[spot] = channel
        sorted_ref[spot] = coef_ref[channel]


def order_channels(slots, cells, channel_term, channel_out, coefs):
    channels = coefs.shape[0]
    smem = pl.BlockSpec(memory_space=pltpu.SMEM)
    return pl.pallas_call(
        functools.partial(order_kernel, slots),
        out_shape=(
            jax.ShapeDtypeStruct((2 * channels + 2 * cells,), jnp.int32),
            jax.ShapeDtypeStruct((channels,), F32),
        ),
        in_specs=[smem] * 3,
        out_specs=(smem, smem),
        scratch_shapes=[pltpu.SMEM((cells,), jnp.int32)],
    )(channel_term, channel_out, coefs)


def line_kernel(
    sectors, moved, dims_ref, table_ref, coef_ref, state_ref, right_ref, left_ref, out_ref,
    left_all, running, summed,
    state_all, masked, gathered, comb, comb_end, acc, acc_end,
    stage, landed, stage_end, landed_end, back, back_landed,
    local_sems, state_send, state_recv, own_send, relay_send, right_recv,
    end_send, end_recv, part_send, part_recv, part_end_send, part_end_recv, back_sems,
):
    terms, width, cols = right_ref.shape
    rows = state_ref.shape[0]
    slots = comb.shape[1] // rows
    me = lax.axis_index("pan")
    sector = lax.axis_index("sec")
    is_mid = (me == 1) | (me == 2)
    is_end = jnp.logical_not(is_mid)
    near_end = jnp.where(me <= 1, 0, 3)
    other_mid = jnp.where(me <= 1, 2, 1)
    far_end = 3 - near_end
    near_mid = jnp.where(me <= 1, 1, 2)

    def remote(src, dst, send, recv, where, axis="pan"):
        return pltpu.make_async_remote_copy(
            src_ref=src, dst_ref=dst, send_sem=send, recv_sem=recv,
            device_id={axis: where}, device_id_type=pl.DeviceIdType.MESH,
        )

    def state_copy(shift):
        where = lax.rem(me + shift, 4)
        spot = state_all.at[me]
        return remote(state_ref, spot, state_send.at[shift], state_recv.at[me], where)

    def state_wait(owner):
        remote(state_ref, state_all.at[owner], state_send.at[0], state_recv.at[owner], me).wait_recv()

    def own_copy(way, term, where):
        return remote(
            right_ref.at[term], gathered.at[me, term],
            own_send.at[way, term], right_recv.at[me, term], where,
        )

    def relay_copy(way, owner, term, where):
        block = gathered.at[owner, term]
        return remote(block, block, relay_send.at[way, term], right_recv.at[owner, term], where)

    def end_copy(term):
        return remote(comb.at[term], comb_end.at[term], end_send.at[term], end_recv.at[term], near_mid)

    def arrived(owner, term):
        block = gathered.at[owner, term]
        remote(block, block, relay_send.at[0, term], right_recv.at[owner, term], me).wait_recv()

    def part_copy(index, owner):
        return remote(
            stage.at[index, owner], landed.at[index, owner],
            part_send.at[index, owner], part_recv.at[index, owner], sector + OFFSETS[index], "sec",
        )

    def part_end_copy(index):
        return remote(
            stage_end.at[index], landed_end.at[index],
            part_end_send.at[index], part_end_recv.at[index], sector + OFFSETS[index], "sec",
        )

    def goes(index):
        target = sector + OFFSETS[index]
        return (target >= 0) & (target < sectors)

    def comes(index):
        source = sector - OFFSETS[index]
        return (source >= 0) & (source < sectors)

    for shift in (1, 2, 3):
        state_copy(shift).start()

    @pl.when(is_mid)
    def _():
        @pl.loop(0, terms)
        def _(term):
            own_copy(0, term, other_mid).start()

            @pl.when(term >= moved)
            def _():
                own_copy(1, term, near_end).start()

    @pl.when(is_end)
    def _():
        @pl.loop(0, terms)
        def _(term):
            own_copy(0, term, near_mid).start()

    copies = [
        pltpu.make_async_copy(state_ref, state_all.at[me], local_sems.at[0]),
        pltpu.make_async_copy(right_ref, gathered.at[me], local_sems.at[1]),
        pltpu.make_async_copy(left_ref, left_all, local_sems.at[2]),
    ]
    for copy in copies:
        copy.start()
    acc[...] = jnp.zeros_like(acc)
    acc_end[...] = jnp.zeros_like(acc_end)
    running[...] = jnp.zeros_like(running)
    for copy in copies:
        copy.wait()

    channels = left_all.shape[0]
    cells = terms * slots

    @pl.loop(0, channels)
    def _(step):
        kept = table_ref[channels + step].astype(F32)
        total = running[...] * kept + left_all[table_ref[step]].astype(F32) * coef_ref[step]
        running[...] = total
        summed[step] = total.astype(BF16)

    @pl.loop(0, terms)
    def _(term):
        for slot in range(slots):
            cell = term * slots + slot
            filled = table_ref[2 * channels + cells + cell].astype(F32)
            value = summed[table_ref[2 * channels + cell]].astype(F32) * filled
            comb[term, slot * rows:(slot + 1) * rows, :] = value.astype(BF16)

    for shift in (1, 2, 3):
        state_wait(lax.rem(me + shift, 4))

    @pl.when(is_end)
    def _():
        @pl.loop(0, moved)
        def _(term):
            end_copy(term).start()

    live = dims_ref[0]
    inside_col = lax.broadcasted_iota(jnp.int32, (rows, width), 1) < live
    for owner in range(4):
        row = lax.broadcasted_iota(jnp.int32, (rows, width), 0) + owner * rows
        masked[owner * rows:(owner + 1) * rows, :] = jnp.where(
            inside_col & (row < live), state_all[owner].astype(F32), 0.0
        ).astype(BF16)

    def multiply(owner, term, left, total):
        block = jnp.dot(masked[...], gathered[owner, term], preferred_element_type=F32).astype(BF16)
        total[owner] += jnp.dot(left[term], block, preferred_element_type=F32)

    def send_parts(owner):
        for index in range(4):
            slot = OFFSETS[index] + 2

            @pl.when(goes(index))
            def _():
                stage[index, owner] = acc[owner, slot * rows:(slot + 1) * rows, :].astype(BF16)
                part_copy(index, owner).start()

    @pl.when(is_mid)
    def _():
        @pl.loop(0, terms)
        def _(term):
            arrived(other_mid, term)

            @pl.when(term >= moved)
            def _():
                relay_copy(0, other_mid, term, near_end).start()

            arrived(near_end, term)
            relay_copy(1, near_end, term, other_mid).start()

            @pl.loop(0, 3)
            def _(which):
                owner = jnp.where(which == 0, me, jnp.where(which == 1, other_mid, near_end))
                multiply(owner, term, comb, acc)

        @pl.loop(0, 3)
        def _(which):
            send_parts(jnp.where(which == 0, me, jnp.where(which == 1, other_mid, near_end)))

        @pl.loop(0, terms)
        def _(term):
            arrived(far_end, term)

            @pl.when(term >= moved)
            def _():
                relay_copy(2, far_end, term, near_end).start()

            multiply(far_end, term, comb, acc)

        send_parts(far_end)

        @pl.loop(0, moved)
        def _(term):
            remote(comb.at[term], comb_end.at[term], end_send.at[term], end_recv.at[term], me).wait_recv()

            @pl.loop(0, 4)
            def _(owner):
                multiply(owner, term, comb_end, acc_end)

        for index in range(4):
            slot = OFFSETS[index] + 2

            @pl.when(goes(index))
            def _():
                stage_end[index] = acc_end[:, slot * rows:(slot + 1) * rows, :].astype(BF16)
                part_end_copy(index).start()

        for index in range(4):
            @pl.when(comes(index))
            def _():
                part_end_copy(index).wait_recv()
                acc_end[:, 2 * rows:3 * rows, :] += landed_end[index].astype(F32)

        back[...] = acc_end[:, 2 * rows:3 * rows, :].astype(BF16)
        remote(back, back_landed, back_sems.at[0], back_sems.at[1], near_end).start()

    @pl.when(is_end)
    def _():
        turn = jnp.where(me == 0, 1, -1)

        @pl.loop(0, 4)
        def _(rank):
            owner = me + turn * rank

            @pl.loop(moved, terms)
            def _(term):
                @pl.when(rank > 0)
                def _():
                    arrived(owner, term)

                multiply(owner, term, comb, acc)

            send_parts(owner)

    for index in range(4):
        @pl.when(comes(index))
        def _():
            @pl.loop(0, 4)
            def _(owner):
                part_copy(index, owner).wait_recv()
                acc[owner, 2 * rows:3 * rows, :] += landed[index, owner].astype(F32)

    @pl.when(is_end)
    def _():
        remote(back, back_landed, back_sems.at[0], back_sems.at[1], me).wait_recv()
        acc[:, 2 * rows:3 * rows, :] += back_landed[...].astype(F32)

    for owner in range(4):
        out_ref[:, owner * cols:(owner + 1) * cols] = acc[owner, 2 * rows:3 * rows, :]

    for shift in (1, 2, 3):
        state_copy(shift).wait_send()
    for index in range(4):
        @pl.when(goes(index))
        def _():
            @pl.loop(0, 4)
            def _(owner):
                part_copy(index, owner).wait_send()

            @pl.when(is_mid)
            def _():
                part_end_copy(index).wait_send()

    @pl.when(is_mid)
    def _():
        @pl.loop(0, terms)
        def _(term):
            own_copy(0, term, other_mid).wait_send()
            relay_copy(1, near_end, term, other_mid).wait_send()

            @pl.when(term >= moved)
            def _():
                own_copy(1, term, near_end).wait_send()
                relay_copy(0, other_mid, term, near_end).wait_send()
                relay_copy(2, far_end, term, near_end).wait_send()

        remote(back, back_landed, back_sems.at[0], back_sems.at[1], near_end).wait_send()

    @pl.when(is_end)
    def _():
        @pl.loop(0, terms)
        def _(term):
            own_copy(0, term, near_mid).wait_send()

        @pl.loop(0, moved)
        def _(term):
            end_copy(term).wait_send()


def line_apply(sectors, slots, dims, table, coefs, state, right, left):
    terms, width, cols = right.shape
    rows = state.shape[0]
    moved = max(1, terms // 4)
    tall = slots * rows
    dma = pltpu.SemaphoreType.DMA
    any_space = pl.BlockSpec(memory_space=pl.ANY)
    return pl.pallas_call(
        functools.partial(line_kernel, sectors, moved),
        out_shape=jax.ShapeDtypeStruct((rows, width), F32),
        in_specs=[pl.BlockSpec(memory_space=pltpu.SMEM)] * 3 + [any_space] * 3,
        out_specs=pl.BlockSpec(memory_space=pltpu.VMEM),
        scratch_shapes=[
            pltpu.VMEM(left.shape, BF16),
            pltpu.VMEM((rows, width), F32),
            pltpu.VMEM(left.shape, BF16),
            pltpu.VMEM((4, rows, width), BF16),
            pltpu.VMEM((width, width), BF16),
            pltpu.VMEM((4, terms, width, cols), BF16),
            pltpu.VMEM((terms, tall, width), BF16),
            pltpu.VMEM((moved, tall, width), BF16),
            pltpu.VMEM((4, tall, cols), F32),
            pltpu.VMEM((4, tall, cols), F32),
            pltpu.VMEM((4, 4, rows, cols), BF16),
            pltpu.VMEM((4, 4, rows, cols), BF16),
            pltpu.VMEM((4, 4, rows, cols), BF16),
            pltpu.VMEM((4, 4, rows, cols), BF16),
            pltpu.VMEM((4, rows, cols), BF16),
            pltpu.VMEM((4, rows, cols), BF16),
            dma((3,)), dma((4,)), dma((4,)),
            dma((2, terms)), dma((3, terms)), dma((4, terms)),
            dma((moved,)), dma((moved,)),
            dma((4, 4)), dma((4, 4)), dma((4,)), dma((4,)), dma((2,)),
        ],
        compiler_params=pltpu.CompilerParams(
            has_side_effects=True, vmem_limit_bytes=56 * 2**20
        ),
    )(dims, table, coefs, state, right, left)


def passed_along(value, axis, steps):
    count = lax.axis_size(axis)
    first, last = (max(0, -steps), min(count, count - steps))
    return lax.ppermute(value, axis, [(source, source + steps) for source in range(first, last)])


def gathered_apply(sector, live_dim, wave, right, combined, rows, slots):
    width = wave.shape[1]
    terms = right.shape[0]
    whole_state = lax.all_gather(wave, "pan", axis=0, tiled=True)
    indices = lax.iota(jnp.int32, width)
    inside = (indices[:, None] < live_dim) & (indices[None, :] < live_dim)
    masked = jnp.where(inside, whole_state, jnp.zeros((), BF16))
    right_full = lax.all_gather(right, "pan", axis=2, tiled=True)
    term_full = jnp.einsum("ik,wkq->wiq", masked, right_full, preferred_element_type=F32).astype(BF16)
    parts = jnp.einsum(
        "wjri,wiq->jrq", combined.reshape(terms, slots, rows, width), term_full,
        preferred_element_type=F32,
    )
    collected = parts[2]
    for offset in OFFSETS:
        collected = collected + passed_along(parts[offset + 2], "sec", offset)
    return collected


def on_device(
    wave_state, right_blocks, left_blocks, coupling, channel_term, channel_out, sector_dims
):
    rows, width = wave_state.shape[1:]
    terms = right_blocks.shape[1]
    slots = 5
    sector = lax.axis_index("sec")
    live_dim = sector_dims[0]
    cells = channel_term * slots + channel_out - sector + 2
    coefs = coupling.astype(F32)
    if lax.axis_size("pan") == 4 and right_blocks.shape[3] % 128 == 0:
        table, ordered = order_channels(slots, terms * slots, channel_term, channel_out, coefs)
        collected = line_apply(
            lax.axis_size("sec"), slots, sector_dims, table, ordered,
            wave_state[0], right_blocks[0], left_blocks,
        )
    else:
        combined = combine(cells, coefs, left_blocks, terms * slots)
        collected = gathered_apply(
            sector, live_dim, wave_state[0], right_blocks[0], combined, rows, slots
        )
    indices = lax.iota(jnp.int32, width)
    row_ids = lax.axis_index("pan") * rows + lax.iota(jnp.int32, rows)
    kept_mask = (row_ids[:, None] < live_dim) & (indices[None, :] < live_dim)
    return jnp.where(kept_mask, collected, jnp.zeros((), F32))[None]


def solution(mesh):
    return jax.shard_map(
        on_device,
        mesh=mesh,
        in_specs=(
            P("sec", "pan", None),
            P("sec", None, None, "pan"),
            P("sec", "pan", None),
            P("sec"),
            P("sec"),
            P("sec"),
            P("sec"),
        ),
        out_specs=P("sec", "pan", None),
        check_vma=False,
    )
```
